32 devices in a mesh: smp: 8 (over z, y), var: 4 (over x, core).
Axes of the slice: x: 2, y: 2, z: 4, core: 2. Of those that a mesh axis runs over, the one named last changes fastest.
Arguments:
- dosage: int32 [512, 2048], P('smp', 'var'), may hold values from -2147483648 to 2147483647, as said below
- shares_init: float32 [12, 8192], P(None, ('smp', 'var')), may hold values from 0.1 to 1
- freqs_init: float32 [12, 2048], P(None, ('var', 'smp')), may hold values from 0.019 to 0.981
Outputs:
- shares: float32 [12, 8192], P(None, ('smp', 'var'))
- freqs: float32 [12, 2048], P(None, ('var', 'smp'))
The draws below stay inside these ranges and needn't reach their ends.
Inputs may be any that keep to these rules, and one draw needn't show every extreme that they name: Every 2-bit code in a word of dosage is 0, 1, 2 or 3, and 3 marks a missing genotype.
All inputs are finite; a program needn't handle non-finite values.
Results may differ from the reference program's by a relative error of at most 0.0003.
Values sent between devices are 32-bit elements; how exact they have to be, the bound alone decides.
A program may use at most 64 MiB of HBM per device.

```python
import math
import jax
import jax.numpy as jnp
from jax import lax

K = 12
ITERS = 2
R_DEV = 1024
N = 8192
M = 2048


def planted_weights(key):
    weight_key = jax.random.fold_in(key, 201)
    cube_base = jax.random.randint(jax.random.fold_in(weight_key, 1), (K, N), 0, 16, dtype=jnp.int32)
    leading = jax.random.randint(jax.random.fold_in(weight_key, 2), (N,), 0, K, dtype=jnp.int32)
    boost = jnp.where(jnp.arange(K, dtype=jnp.int32)[:, None] == leading[None, :], 20000, 0)
    return cube_base * cube_base * cube_base + 1 + boost


def planted_levels(key):
    level_key = jax.random.fold_in(key, 202)
    spread = jax.random.randint(jax.random.fold_in(level_key, 1), (K, M), 0, 992, dtype=jnp.int32)
    flipped = jax.random.randint(jax.random.fold_in(level_key, 2), (K, M), 0, 2, dtype=jnp.int32)
    lower = 16 + spread * spread // 992
    return jnp.where(flipped == 1, 1024 - lower, lower)


def draw_dosage(key, part):
    weights = planted_weights(key)
    levels = planted_levels(key)
    grouped = weights.reshape(K, N // 16, 16)
    genotype_key = jax.random.fold_in(key, 203)

    def add_codes(position, packed):
        picked = lax.dynamic_index_in_dim(grouped, position, 2, keepdims=False)
        numerator = jnp.dot(picked.T, levels)
        denominator = jnp.sum(picked, axis=0) * 1024
        sample_key = jax.random.fold_in(genotype_key, position)
        limit = jnp.broadcast_to(denominator[:, None], numerator.shape)
        first_draw = jax.random.randint(jax.random.fold_in(sample_key, 1), numerator.shape, 0, limit, dtype=jnp.int32)
        second_draw = jax.random.randint(jax.random.fold_in(sample_key, 2), numerator.shape, 0, limit, dtype=jnp.int32)
        alleles = (first_draw < numerator).astype(jnp.int32) + (second_draw < numerator).astype(jnp.int32)
        absent = jax.random.randint(jax.random.fold_in(sample_key, 3), numerator.shape, 0, 10, dtype=jnp.int32) == 0
        codes = jnp.where(absent, 3, alleles)
        return jnp.bitwise_or(packed, jnp.left_shift(codes, 2 * position))
    return lax.fori_loop(0, 16, add_codes, jnp.zeros((N // 16, M), jnp.int32))


def draw_freqs_init(key, part):
    levels = planted_levels(key)
    base = levels.astype(jnp.float32) / 1024.0
    noise = jax.random.uniform(jax.random.fold_in(key, 204), (K, M), jnp.float32, 0.05, 0.95)
    return 0.9 * base + 0.1 * noise


def shard_levels(stream_key, dims, cuts, least, high):
    def one(dim, parts):
        heights = jax.random.uniform(jax.random.fold_in(jax.random.fold_in(stream_key, 6), dim), (parts,), jnp.float32, least / len(cuts), high / len(cuts))
        return jnp.repeat(jnp.exp(heights), dims[dim] // parts).reshape((-1,) + (1,) * (len(dims) - dim - 1))

    loudness = one(*cuts[0])
    for cut in cuts[1:]:
        loudness = loudness * one(*cut)
    return loudness


def setup_inputs(seed: int = 0) -> dict:
    key_list = jax.random.split(jax.random.key(seed), 4)
    dosage = draw_dosage(jax.random.fold_in(key_list[3], 71), 0)
    shares_init = jnp.clip(jnp.exp(math.log(1.0) - 2.3025851 * jax.random.uniform(key_list[1], (K, N), jnp.float32) ** shard_levels(key_list[1], (K, N), ((1, 32),), -0.2, 0.2)), 0.1, 1.0)
    freqs_init = draw_freqs_init(jax.random.fold_in(key_list[3], 71), 0)
    return dict(dosage=dosage, shares_init=shares_init, freqs_init=freqs_init)


HIGH = lax.Precision.HIGHEST


def unpack_codes(packed):
    shifts = 2 * jnp.arange(16, dtype=jnp.int32)
    codes = jnp.bitwise_and(jnp.right_shift(packed[:, None, :], shifts[None, :, None]), 3)
    return codes.reshape(packed.shape[0] * 16, packed.shape[1])


def expect_sums(packed, shares_block, freqs_block):
    codes = unpack_codes(packed)
    live = (codes < 3).astype(jnp.float32)
    allele_f = live * codes.astype(jnp.float32)
    probs = jnp.einsum("kn,km->nm", shares_block, freqs_block, precision=HIGH)
    ratio_alt = allele_f / probs
    ratio_ref = (2.0 * live - allele_f) / (1.0 - probs)
    sum_q = jnp.einsum("km,nm->kn", freqs_block, ratio_alt, precision=HIGH) + jnp.einsum("km,nm->kn", 1.0 - freqs_block, ratio_ref, precision=HIGH)
    sum_a = jnp.einsum("kn,nm->km", shares_block, ratio_alt, precision=HIGH)
    sum_b = jnp.einsum("kn,nm->km", shares_block, ratio_ref, precision=HIGH)
    return sum_q, sum_a, sum_b


def renew_shares(shares_block, sum_q):
    numer = shares_block * sum_q
    return (numer + 0.5) / (jnp.sum(numer, axis=0, keepdims=True) + 0.5 * shares_block.shape[0])


def renew_freqs(freqs_block, sum_a, sum_b):
    alt_part = freqs_block * sum_a
    ref_part = (1.0 - freqs_block) * sum_b
    return (alt_part + 0.5) / (alt_part + ref_part + 1.0)


def reference(dosage, shares_init, freqs_init):
    shares_now = shares_init / jnp.sum(shares_init, axis=0, keepdims=True)
    freqs_now = freqs_init
    blocks = dosage.shape[0] * 16 // R_DEV
    packed_blocks = dosage.reshape(blocks, R_DEV // 16, dosage.shape[1])
    for iteration in range(ITERS):
        share_blocks = shares_now.reshape(K, blocks, R_DEV).transpose(1, 0, 2)

        def one_block(carry, items):
            sum_q, sum_a, sum_b = expect_sums(items[0], items[1], freqs_now)
            return (carry[0] + sum_a, carry[1] + sum_b), sum_q

        start = (jnp.zeros(freqs_now.shape, jnp.float32), jnp.zeros(freqs_now.shape, jnp.float32))
        totals, sums_q = lax.scan(one_block, start, (packed_blocks, share_blocks))
        sum_q = sums_q.transpose(1, 0, 2).reshape(K, shares_now.shape[1])
        new_shares = renew_shares(shares_now, sum_q)
        freqs_now = renew_freqs(freqs_now, totals[0], totals[1])
        shares_now = new_shares
    return shares_now, freqs_now
```

```python
import functools

import jax
import jax.numpy as jnp
from jax import lax
from jax.experimental import pallas as pl
from jax.experimental.pallas import tpu as pltpu
from jax.sharding import PartitionSpec as P

ITERS = 2
CODES = 16
PAD = 16
F32 = jnp.float32
BF16 = jnp.bfloat16


def split(x, pieces):
    out = []
    for _ in range(pieces):
        piece = x.astype(BF16)
        out.append(piece)
        x = x - piece.astype(F32)
    return out


def dot(a, b):
    return jnp.dot(a, b, preferred_element_type=F32)


def em_kernel(
    nv, ns, dosage_hbm, shares_ref, freqs_ref, shares_out, freqs_out,
    dosage_ref, q_slots, f_slots, sq_send, sq_recv, sf_send, sf_recv,
    q_pad, f_pad, qt_ref, q2_ref, fs_ref, fta_ref, ftb_ref,
    load_sem, q_ss, q_rs, f_ss, f_rs, sq_ss, sq_rs, sf_ss, sf_rs,
):
    iv, js = lax.axis_index("var"), lax.axis_index("smp")
    pops, ws = shares_ref.shape
    wf = freqs_ref.shape[1]
    words, variants = dosage_ref.shape
    samples = words * CODES

    load = pltpu.make_async_copy(dosage_hbm, dosage_ref, load_sem)
    load.start()

    def var_peer(d):
        return lax.rem(iv + d, nv)

    def smp_peer(d):
        return lax.rem(js + d, ns)

    barrier = pltpu.get_barrier_semaphore()
    for d in range(1, ns):
        pl.semaphore_signal(barrier, inc=1, device_id=(smp_peer(d), iv), device_id_type=pl.DeviceIdType.MESH)
    for d in range(1, nv):
        pl.semaphore_signal(barrier, inc=1, device_id=(js, var_peer(d)), device_id_type=pl.DeviceIdType.MESH)

    q_own = shares_ref[...]
    q_own = q_own / jnp.sum(q_own, axis=0, keepdims=True)
    f_own = freqs_ref[...]
    q_pad[...] = jnp.zeros_like(q_pad)
    f_pad[...] = jnp.zeros_like(f_pad)
    q_slots[0, iv] = q_own
    f_slots[0, js] = f_own
    pl.semaphore_wait(barrier, ns - 1 + nv - 1)

    def copies_smp(src_of, dst, it, ss, rs):
        made = []
        for d in range(1, ns):
            to, frm = smp_peer(d), smp_peer(ns - d)
            send = pltpu.make_async_remote_copy(
                src_ref=src_of(to), dst_ref=dst.at[it, js], send_sem=ss.at[it, to], recv_sem=rs.at[it, js],
                device_id=(to, iv), device_id_type=pl.DeviceIdType.MESH)
            recv = pltpu.make_async_remote_copy(
                src_ref=src_of(to), dst_ref=dst.at[it, frm], send_sem=ss.at[it, to], recv_sem=rs.at[it, frm],
                device_id=(frm, iv), device_id_type=pl.DeviceIdType.MESH)
            made.append((send, recv))
        return made

    def copies_var(src_of, dst, it, ss, rs):
        made = []
        for d in range(1, nv):
            to, frm = var_peer(d), var_peer(nv - d)
            send = pltpu.make_async_remote_copy(
                src_ref=src_of(to), dst_ref=dst.at[it, iv], send_sem=ss.at[it, to], recv_sem=rs.at[it, iv],
                device_id=(js, to), device_id_type=pl.DeviceIdType.MESH)
            recv = pltpu.make_async_remote_copy(
                src_ref=src_of(to), dst_ref=dst.at[it, frm], send_sem=ss.at[it, to], recv_sem=rs.at[it, frm],
                device_id=(js, frm), device_id_type=pl.DeviceIdType.MESH)
            made.append((send, recv))
        return made

    def start(made):
        for send, _ in made:
            send.start()

    def arrive(made):
        for _, recv in made:
            recv.wait_recv()

    def sent(made):
        for send, _ in made:
            send.wait_send()

    sent_later = []
    for it in range(ITERS):
        last = it + 1 == ITERS
        f_copies = copies_smp(lambda to: f_slots.at[it, js], f_slots, it, f_ss, f_rs)
        q_copies = copies_var(lambda to: q_slots.at[it, iv], q_slots, it, q_ss, q_rs)
        start(f_copies)
        start(q_copies)
        sent_later += [f_copies, q_copies]

        arrive(q_copies)
        for v in range(nv):
            q_pad[0:pops, v * ws:(v + 1) * ws] = q_slots[it, v]
        qh, qm, ql = split(q_pad[...], 3)
        qs = jnp.concatenate([qh, qh, qm, qh, qm, ql, qm, ql], axis=0)
        qt_ref[...] = qs.astype(F32).T.astype(BF16)
        q2_ref[...] = jnp.concatenate([qh, qm], axis=0)
        if it == 0:
            load.wait()

        arrive(f_copies)
        for s in range(ns):
            f_pad[0:pops, s * wf:(s + 1) * wf] = f_slots[it, s]
        f_all = f_pad[...]
        fh, fm, fl = split(f_all, 3)
        gh, gm = split(1.0 - f_all, 2)
        fs_ref[...] = jnp.concatenate([fh, fm, fh, fl, fm, fh, fl, fm], axis=0)
        ft = jnp.concatenate([fh, fm, gh, gm, fh, fm, gh, gm], axis=0).astype(F32).T.astype(BF16)
        fta_ref[...] = ft[:, 0:2 * PAD]
        ftb_ref[...] = ft[:, 2 * PAD:4 * PAD]

        sum_a = jnp.zeros((2 * PAD, variants), F32)
        sum_b = jnp.zeros((2 * PAD, variants), F32)
        sq_parts = []
        rows = 256
        for b in range(samples // rows):
            here = slice(b * rows, (b + 1) * rows)
            packed = dosage_ref[b * rows // CODES:(b + 1) * rows // CODES, :]
            shape3 = (rows // CODES, CODES, variants)
            shifts = 2 * lax.broadcasted_iota(jnp.int32, shape3, 1)
            codes = jnp.bitwise_and(jnp.right_shift(jnp.broadcast_to(packed[:, None, :], shape3), shifts), 3)
            codes = codes.reshape(rows, variants)
            probs = dot(qt_ref[here, :], fs_ref[...])
            rest = 1.0 - probs
            inv = 1.0 / (probs * rest)
            live = codes < 3
            codes_f = codes.astype(F32)
            a = jnp.where(live, codes_f, 0.0) * (rest * inv)
            bb = jnp.where(live, 2.0 - codes_f, 0.0) * (probs * inv)
            ah, al = split(a, 2)
            bh, bl = split(bb, 2)
            q2 = q2_ref[:, here]
            sum_a = sum_a + dot(q2, ah) + dot(q2, al)
            sum_b = sum_b + dot(q2, bh) + dot(q2, bl)
            sq = (dot(ah, fta_ref[...]) + dot(al, fta_ref[...])) + (dot(bh, ftb_ref[...]) + dot(bl, ftb_ref[...]))
            sq_t = sq.T
            sq_parts.append(sq_t[0:PAD] + sq_t[PAD:2 * PAD])
        sum_a = (sum_a[0:PAD] + sum_a[PAD:2 * PAD])[0:pops]
        sum_b = (sum_b[0:PAD] + sum_b[PAD:2 * PAD])[0:pops]
        for s in range(ns):
            cut = slice(s * wf, (s + 1) * wf)
            sf_send[it, s] = jnp.concatenate([sum_a[:, cut], sum_b[:, cut]], axis=1)
        sf_copies = copies_smp(lambda to: sf_send.at[it, to], sf_recv, it, sf_ss, sf_rs)
        start(sf_copies)
        sum_q = jnp.concatenate(sq_parts, axis=1)[0:pops]
        for v in range(nv):
            sq_send[it, v] = sum_q[:, v * ws:(v + 1) * ws]
        sq_copies = copies_var(lambda to: sq_send.at[it, to], sq_recv, it, sq_ss, sq_rs)
        start(sq_copies)
        sent_later += [sf_copies, sq_copies]

        arrive(sq_copies)
        total = sq_send[it, iv]
        for d in range(1, nv):
            total = total + sq_recv[it, var_peer(d)]
        numer = q_own * total
        q_own = (numer + 0.5) / (jnp.sum(numer, axis=0, keepdims=True) + 0.5 * pops)
        if last:
            shares_out[...] = q_own
        else:
            q_slots[it + 1, iv] = q_own

        arrive(sf_copies)
        total = sf_send[it, js]
        for d in range(1, ns):
            total = total + sf_recv[it, smp_peer(d)]
        alt_part = f_own * total[:, 0:wf]
        ref_part = (1.0 - f_own) * total[:, wf:2 * wf]
        f_own = (alt_part + 0.5) / (alt_part + ref_part + 1.0)
        if last:
            freqs_out[...] = f_own
        else:
            f_slots[it + 1, js] = f_own

    for made in sent_later:
        sent(made)


def body(nv, ns, dosage, shares_init, freqs_init):
    pops, ws = shares_init.shape
    wf = freqs_init.shape[1]
    words, variants = dosage.shape
    samples = words * CODES
    vmem = pl.BlockSpec(memory_space=pltpu.VMEM)
    dma = pltpu.SemaphoreType.DMA
    return pl.pallas_call(
        functools.partial(em_kernel, nv, ns),
        out_shape=(
            jax.ShapeDtypeStruct((pops, ws), F32),
            jax.ShapeDtypeStruct((pops, wf), F32),
        ),
        in_specs=[pl.BlockSpec(memory_space=pl.ANY), vmem, vmem],
        out_specs=(vmem, vmem),
        scratch_shapes=[
            pltpu.VMEM((words, variants), jnp.int32),
            pltpu.VMEM((ITERS, nv, pops, ws), F32),
            pltpu.VMEM((ITERS, ns, pops, wf), F32),
            pltpu.VMEM((ITERS, nv, pops, ws), F32),
            pltpu.VMEM((ITERS, nv, pops, ws), F32),
            pltpu.VMEM((ITERS, ns, pops, 2 * wf), F32),
            pltpu.VMEM((ITERS, ns, pops, 2 * wf), F32),
            pltpu.VMEM((PAD, samples), F32),
            pltpu.VMEM((PAD, variants), F32),
            pltpu.VMEM((samples, 8 * PAD), BF16),
            pltpu.VMEM((2 * PAD, samples), BF16),
            pltpu.VMEM((8 * PAD, variants), BF16),
            pltpu.VMEM((variants, 2 * PAD), BF16),
            pltpu.VMEM((variants, 2 * PAD), BF16),
            dma,
            dma((ITERS, nv)), dma((ITERS, nv)),
            dma((ITERS, ns)), dma((ITERS, ns)),
            dma((ITERS, nv)), dma((ITERS, nv)),
            dma((ITERS, ns)), dma((ITERS, ns)),
        ],
        compiler_params=pltpu.CompilerParams(collective_id=0, has_side_effects=True),
        cost_estimate=pl.CostEstimate(flops=200000000, bytes_accessed=400000, transcendentals=1000000),
    )(dosage, shares_init, freqs_init)


def solution(mesh):
    placed = (P("smp", "var"), P(None, ("smp", "var")), P(None, ("var", "smp")))
    return jax.shard_map(
        functools.partial(body, mesh.shape["var"], mesh.shape["smp"]),
        mesh=mesh,
        in_specs=placed,
        out_specs=(P(None, ("smp", "var")), P(None, ("var", "smp"))),
        check_vma=False,
    )
```

```python
import functools

import jax
import jax.numpy as jnp
from jax import lax
from jax.experimental import pallas as pl
from jax.experimental.pallas import tpu as pltpu
from jax.sharding import PartitionSpec as P

ITERS = 2
CODES = 16
PAD = 16
F32 = jnp.float32
BF16 = jnp.bfloat16


def split(x, pieces):
    out = []
    for _ in range(pieces):
        piece = x.astype(BF16)
        out.append(piece)
        x = x - piece.astype(F32)
    return out


def dot(a, b):
    return jnp.dot(a, b, preferred_element_type=F32)


def em_kernel(
    nv, ns, chunk, dosage_hbm, shares_hbm, freqs_hbm, shares_out, freqs_out,
    dosage_ref, shares_ref, freqs_ref, q_slots, f_slots, sq_send, sq_recv, sf_send, sf_recv,
    q_pad, f_pad, qt_ref, q2_ref, fs_ref, fta_ref, ftb_ref,
    load_sem, q_ss, q_rs, f_ss, f_rs, sq_ss, sq_rs, sf_ss, sf_rs,
):
    iv, js = lax.axis_index("var"), lax.axis_index("smp")
    pops, ws = shares_ref.shape
    wf = freqs_ref.shape[1]
    words, variants = dosage_ref.shape
    samples = words * CODES
    chunks = variants // chunk
    per = ns // chunks
    own_chunk, own_place = js // per, lax.rem(js, per)
    mesh_ids = pl.DeviceIdType.MESH

    def chunk_at(t):
        return lax.rem(own_chunk + t, chunks)

    def smp_peer(t, d):
        return chunk_at(t) * per + lax.rem(own_place + d, per)

    def var_peer(d):
        return lax.rem(iv + d, nv)

    smp_peers = [[smp_peer(t, d) for d in range(0 if t else 1, per)] for t in range(chunks)]
    all_smp = [p for t in reversed(range(chunks)) for p in smp_peers[t]]
    var_peers = [var_peer(d) for d in range(1, nv)]

    barrier = pltpu.get_barrier_semaphore()
    for p in all_smp:
        pl.semaphore_signal(barrier, inc=1, device_id=(p, iv), device_id_type=mesh_ids)
    for p in var_peers:
        pl.semaphore_signal(barrier, inc=1, device_id=(js, p), device_id_type=mesh_ids)

    load_q = pltpu.make_async_copy(shares_hbm, shares_ref, load_sem.at[0])
    load_f = pltpu.make_async_copy(freqs_hbm, f_slots.at[0, js], load_sem.at[1])
    load_f2 = pltpu.make_async_copy(freqs_hbm, freqs_ref, load_sem.at[2])
    load_d = pltpu.make_async_copy(dosage_hbm, dosage_ref, load_sem.at[3])
    load_q.start()
    load_f.start()
    load_f2.start()
    load_d.start()
    q_pad[...] = jnp.zeros_like(q_pad)
    f_pad[...] = jnp.zeros_like(f_pad)
    load_q.wait()
    q_own = shares_ref[...]
    q_own = q_own / jnp.sum(q_own, axis=0, keepdims=True)
    q_slots[0, iv] = q_own
    load_f.wait()
    load_f2.wait()
    f_own = freqs_ref[...]
    pl.semaphore_wait(barrier, ns - 1 + nv - 1)

    def smp_copy(src, dst, it, ss, rs, to, slot):
        return pltpu.make_async_remote_copy(
            src_ref=src, dst_ref=dst.at[it, slot], send_sem=ss.at[it, to], recv_sem=rs.at[it, slot],
            device_id=(to, iv), device_id_type=mesh_ids)

    def var_copy(src, dst, it, ss, rs, to, slot):
        return pltpu.make_async_remote_copy(
            src_ref=src, dst_ref=dst.at[it, slot], send_sem=ss.at[it, to], recv_sem=rs.at[it, slot],
            device_id=(js, to), device_id_type=mesh_ids)

    sent = []

    def start(copy):
        copy.start()
        sent.append(copy)

    rows = 256
    blocks = samples // rows
    for it in range(ITERS):
        last = it + 1 == ITERS
        if it == 0:
            for p in all_smp:
                start(smp_copy(f_slots.at[it, js], f_slots, it, f_ss, f_rs, p, js))
            for p in var_peers:
                start(var_copy(q_slots.at[it, iv], q_slots, it, q_ss, q_rs, p, iv))

        for p in var_peers:
            var_copy(q_slots.at[it, iv], q_slots, it, q_ss, q_rs, p, p).wait_recv()
        for v in range(nv):
            q_pad[0:pops, v * ws:(v + 1) * ws] = q_slots[it, v]
        qh, qm, ql = split(q_pad[...], 3)
        qs = jnp.concatenate([qh, qh, qm, qh, qm, ql, qm, ql], axis=0)
        qt_ref[...] = qs.astype(F32).T.astype(BF16)
        q2_ref[...] = jnp.concatenate([qh, qm], axis=0)
        if it == 0:
            load_d.wait()

        sq_acc = [jnp.zeros((rows, 2 * PAD), F32) for _ in range(blocks)]
        for t in range(chunks):
            c = chunk_at(t)
            for p in smp_peers[t]:
                smp_copy(f_slots.at[it, js], f_slots, it, f_ss, f_rs, p, p).wait_recv()
            for i in range(per):
                f_pad[0:pops, i * wf:(i + 1) * wf] = f_slots[it, c * per + i]
            f_all = f_pad[...]
            fh, fm, fl = split(f_all, 3)
            gh, gm = split(1.0 - f_all, 2)
            fs_ref[...] = jnp.concatenate([fh, fm, fh, fl, fm, fh, fl, fm], axis=0)
            ft = jnp.concatenate([fh, fm, gh, gm, fh, fm, gh, gm], axis=0).astype(F32).T.astype(BF16)
            fta_ref[...] = ft[:, 0:2 * PAD]
            ftb_ref[...] = ft[:, 2 * PAD:4 * PAD]

            sum_a = jnp.zeros((2 * PAD, chunk), F32)
            sum_b = jnp.zeros((2 * PAD, chunk), F32)
            lanes = pl.ds(pl.multiple_of(c * chunk, chunk), chunk)
            for b in range(blocks):
                here = slice(b * rows, (b + 1) * rows)
                packed = dosage_ref[b * rows // CODES:(b + 1) * rows // CODES, lanes]
                shape3 = (rows // CODES, CODES, chunk)
                shifts = 2 * lax.broadcasted_iota(jnp.int32, shape3, 1)
                codes = jnp.bitwise_and(jnp.right_shift(jnp.broadcast_to(packed[:, None, :], shape3), shifts), 3)
                codes = codes.reshape(rows, chunk)
                probs = dot(qt_ref[here, :], fs_ref[...])
                rest = 1.0 - probs
                inv = 1.0 / (probs * rest)
                live = codes < 3
                codes_f = codes.astype(F32)
                a = jnp.where(live, codes_f, 0.0) * (rest * inv)
                bb = jnp.where(live, 2.0 - codes_f, 0.0) * (probs * inv)
                ah, al = split(a, 2)
                bh, bl = split(bb, 2)
                q2 = q2_ref[:, here]
                sum_a = sum_a + dot(q2, ah) + dot(q2, al)
                sum_b = sum_b + dot(q2, bh) + dot(q2, bl)
                sq_acc[b] = sq_acc[b] + (dot(ah, fta_ref[...]) + dot(al, fta_ref[...])) + (
                    dot(bh, ftb_ref[...]) + dot(bl, ftb_ref[...]))
            sum_a = (sum_a[0:PAD] + sum_a[PAD:2 * PAD])[0:pops]
            sum_b = (sum_b[0:PAD] + sum_b[PAD:2 * PAD])[0:pops]
            for i in range(per):
                cut = slice(i * wf, (i + 1) * wf)
                sf_send[it, c * per + i] = jnp.concatenate([sum_a[:, cut], sum_b[:, cut]], axis=1)
            for p in smp_peers[t]:
                start(smp_copy(sf_send.at[it, p], sf_recv, it, sf_ss, sf_rs, p, js))

        sq_t = [x.T for x in sq_acc]
        sum_q = jnp.concatenate([x[0:PAD] + x[PAD:2 * PAD] for x in sq_t], axis=1)[0:pops]
        for v in range(nv):
            sq_send[it, v] = sum_q[:, v * ws:(v + 1) * ws]
        for p in var_peers:
            start(var_copy(sq_send.at[it, p], sq_recv, it, sq_ss, sq_rs, p, iv))

        total = sq_send[it, iv]
        for p in var_peers:
            var_copy(sq_send.at[it, p], sq_recv, it, sq_ss, sq_rs, p, p).wait_recv()
            total = total + sq_recv[it, p]
        numer = q_own * total
        q_own = (numer + 0.5) / (jnp.sum(numer, axis=0, keepdims=True) + 0.5 * pops)
        if last:
            shares_out[...] = q_own
        else:
            q_slots[it + 1, iv] = q_own
            for p in var_peers:
                start(var_copy(q_slots.at[it + 1, iv], q_slots, it + 1, q_ss, q_rs, p, iv))

        total = sf_send[it, js]
        for t in range(chunks):
            for p in smp_peers[t]:
                smp_copy(sf_send.at[it, p], sf_recv, it, sf_ss, sf_rs, p, p).wait_recv()
                total = total + sf_recv[it, p]
        alt_part = f_own * total[:, 0:wf]
        ref_part = (1.0 - f_own) * total[:, wf:2 * wf]
        f_own = (alt_part + 0.5) / (alt_part + ref_part + 1.0)
        if last:
            freqs_out[...] = f_own
        else:
            f_slots[it + 1, js] = f_own
            for p in all_smp:
                start(smp_copy(f_slots.at[it + 1, js], f_slots, it + 1, f_ss, f_rs, p, js))

    for copy in sent:
        copy.wait_send()


def hand_out(shares_ref, freqs_ref, shares_out, freqs_out):
    shares_out[...] = shares_ref[...]
    freqs_out[...] = freqs_ref[...]


def body(nv, ns, dosage, shares_init, freqs_init):
    pops, ws = shares_init.shape
    wf = freqs_init.shape[1]
    words, variants = dosage.shape
    samples = words * CODES
    chunk = variants // 2
    vmem = pl.BlockSpec(memory_space=pltpu.VMEM)
    hbm = pl.BlockSpec(memory_space=pl.ANY)
    dma = pltpu.SemaphoreType.DMA
    shapes = (jax.ShapeDtypeStruct((pops, ws), F32), jax.ShapeDtypeStruct((pops, wf), F32))
    shares, freqs = pl.pallas_call(
        functools.partial(em_kernel, nv, ns, chunk),
        out_shape=shapes,
        in_specs=[hbm, hbm, hbm],
        out_specs=(vmem, vmem),
        scratch_shapes=[
            pltpu.VMEM((words, variants), jnp.int32),
            pltpu.VMEM((pops, ws), F32),
            pltpu.VMEM((pops, wf), F32),
            pltpu.VMEM((ITERS, nv, pops, ws), F32),
            pltpu.VMEM((ITERS, ns, pops, wf), F32),
            pltpu.VMEM((ITERS, nv, pops, ws), F32),
            pltpu.VMEM((ITERS, nv, pops, ws), F32),
            pltpu.VMEM((ITERS, ns, pops, 2 * wf), F32),
            pltpu.VMEM((ITERS, ns, pops, 2 * wf), F32),
            pltpu.VMEM((PAD, samples), F32),
            pltpu.VMEM((PAD, chunk), F32),
            pltpu.VMEM((samples, 8 * PAD), BF16),
            pltpu.VMEM((2 * PAD, samples), BF16),
            pltpu.VMEM((8 * PAD, chunk), BF16),
            pltpu.VMEM((chunk, 2 * PAD), BF16),
            pltpu.VMEM((chunk, 2 * PAD), BF16),
            dma((4,)),
            dma((ITERS, nv)), dma((ITERS, nv)),
            dma((ITERS, ns)), dma((ITERS, ns)),
            dma((ITERS, nv)), dma((ITERS, nv)),
            dma((ITERS, ns)), dma((ITERS, ns)),
        ],
        compiler_params=pltpu.CompilerParams(collective_id=0, has_side_effects=True),
        cost_estimate=pl.CostEstimate(flops=200000000, bytes_accessed=400000, transcendentals=1000000),
    )(dosage, shares_init, freqs_init)
    return pl.pallas_call(
        hand_out, out_shape=shapes, in_specs=[vmem, vmem], out_specs=(vmem, vmem),
    )(shares, freqs)


def solution(mesh):
    placed = (P("smp", "var"), P(None, ("smp", "var")), P(None, ("var", "smp")))
    return jax.shard_map(
        functools.partial(body, mesh.shape["var"], mesh.shape["smp"]),
        mesh=mesh,
        in_specs=placed,
        out_specs=(P(None, ("smp", "var")), P(None, ("var", "smp"))),
        check_vma=False,
    )
```

```python
import functools

import jax
import jax.numpy as jnp
from jax import lax
from jax.experimental import pallas as pl
from jax.experimental.pallas import tpu as pltpu
from jax.sharding import PartitionSpec as P

ITERS = 2
CODES = 16
PAD = 16
F32 = jnp.float32
BF16 = jnp.bfloat16


def split(x, pieces):
    out = []
    for _ in range(pieces):
        piece = x.astype(BF16)
        out.append(piece)
        x = x - piece.astype(F32)
    return out


def dot(a, b):
    return jnp.dot(a, b, preferred_element_type=F32)


def em_kernel(
    nv, ns, chunk, dosage_hbm, shares_hbm, freqs_hbm, shares_out, freqs_out,
    dosage_ref, shares_ref, freqs_ref, q_slots, f_slots, sq_send, sq_recv, sf_send, sf_recv,
    q_pad, f_pad, qt_ref, q2_ref, fs_ref, fgs_ref,
    load_sem, q_ss, q_rs, f_ss, f_rs, sq_ss, sq_rs, sf_ss, sf_rs,
):
    iv, js = lax.axis_index("var"), lax.axis_index("smp")
    pops, ws = shares_ref.shape
    wf = freqs_ref.shape[1]
    words, variants = dosage_ref.shape
    samples = words * CODES
    chunks = variants // chunk
    per = ns // chunks
    own_chunk, own_place = js // per, lax.rem(js, per)
    mesh_ids = pl.DeviceIdType.MESH

    def chunk_at(t):
        return lax.rem(own_chunk + t, chunks)

    def smp_peer(t, d):
        return chunk_at(t) * per + lax.rem(own_place + d, per)

    def var_peer(d):
        return lax.rem(iv + d, nv)

    smp_peers = [[smp_peer(t, d) for d in range(0 if t else 1, per)] for t in range(chunks)]
    all_smp = [p for t in reversed(range(chunks)) for p in smp_peers[t]]
    var_peers = [var_peer(d) for d in range(1, nv)]

    barrier = pltpu.get_barrier_semaphore()
    for p in all_smp:
        pl.semaphore_signal(barrier, inc=1, device_id=(p, iv), device_id_type=mesh_ids)
    for p in var_peers:
        pl.semaphore_signal(barrier, inc=1, device_id=(js, p), device_id_type=mesh_ids)

    load_q = pltpu.make_async_copy(shares_hbm, shares_ref, load_sem.at[0])
    load_f = pltpu.make_async_copy(freqs_hbm, f_slots.at[0, js], load_sem.at[1])
    load_f2 = pltpu.make_async_copy(freqs_hbm, freqs_ref, load_sem.at[2])
    load_d = pltpu.make_async_copy(dosage_hbm, dosage_ref, load_sem.at[3])
    load_q.start()
    load_f.start()
    load_f2.start()
    load_d.start()
    q_pad[...] = jnp.zeros_like(q_pad)
    f_pad[...] = jnp.zeros_like(f_pad)
    load_q.wait()
    q_own = shares_ref[...]
    q_own = q_own / jnp.sum(q_own, axis=0, keepdims=True)
    q_slots[0, iv] = q_own
    load_f.wait()
    load_f2.wait()
    f_own = freqs_ref[...]
    pl.semaphore_wait(barrier, ns - 1 + nv - 1)

    def smp_copy(src, dst, it, ss, rs, to, slot):
        return pltpu.make_async_remote_copy(
            src_ref=src, dst_ref=dst.at[it, slot], send_sem=ss.at[it, to], recv_sem=rs.at[it, slot],
            device_id=(to, iv), device_id_type=mesh_ids)

    def var_copy(src, dst, it, ss, rs, to, slot):
        return pltpu.make_async_remote_copy(
            src_ref=src, dst_ref=dst.at[it, slot], send_sem=ss.at[it, to], recv_sem=rs.at[it, slot],
            device_id=(js, to), device_id_type=mesh_ids)

    sent = []

    def start(copy):
        copy.start()
        sent.append(copy)

    rows = 512
    blocks = samples // rows
    for it in range(ITERS):
        last = it + 1 == ITERS
        if it == 0:
            for p in all_smp:
                start(smp_copy(f_slots.at[it, js], f_slots, it, f_ss, f_rs, p, js))
            for p in var_peers:
                start(var_copy(q_slots.at[it, iv], q_slots, it, q_ss, q_rs, p, iv))

        for p in var_peers:
            var_copy(q_slots.at[it, iv], q_slots, it, q_ss, q_rs, p, p).wait_recv()
        for v in range(nv):
            q_pad[0:pops, v * ws:(v + 1) * ws] = q_slots[it, v]
        qh, qm, ql = split(q_pad[...], 3)
        qs = jnp.concatenate([qh, qh, qm, qh, qm, ql, qm, ql], axis=0)
        qt_ref[...] = qs.astype(F32).T.astype(BF16)
        q2_ref[...] = jnp.concatenate([qh, qm], axis=0)
        if it == 0:
            load_d.wait()

        sq_acc = [jnp.zeros((2 * PAD, rows), F32) for _ in range(blocks)]
        for t in range(chunks):
            c = chunk_at(t)
            for p in smp_peers[t]:
                smp_copy(f_slots.at[it, js], f_slots, it, f_ss, f_rs, p, p).wait_recv()
            for i in range(per):
                f_pad[0:pops, i * wf:(i + 1) * wf] = f_slots[it, c * per + i]
            f_all = f_pad[...]
            fh, fm, fl = split(f_all, 3)
            gh, gm = split(1.0 - f_all, 2)
            fs_ref[...] = jnp.concatenate([fh, fm, fh, fl, fm, fh, fl, fm], axis=0)
            fpair = jnp.concatenate([fh, fm], axis=0)
            gpair = jnp.concatenate([gh, gm], axis=0)
            fgs_ref[...] = jnp.concatenate([fpair, fpair, gpair, gpair], axis=1)

            sum_a = jnp.zeros((2 * PAD, chunk), F32)
            sum_b = jnp.zeros((2 * PAD, chunk), F32)
            lanes = pl.ds(pl.multiple_of(c * chunk, chunk), chunk)
            for b in range(blocks):
                here = slice(b * rows, (b + 1) * rows)
                packed = dosage_ref[b * rows // CODES:(b + 1) * rows // CODES, lanes]
                shape3 = (rows // CODES, CODES, chunk)
                shifts = 2 * lax.broadcasted_iota(jnp.int32, shape3, 1)
                codes = jnp.bitwise_and(jnp.right_shift(jnp.broadcast_to(packed[:, None, :], shape3), shifts), 3)
                codes = codes.reshape(rows, chunk)
                probs = dot(qt_ref[here, :], fs_ref[...])
                rest = 1.0 - probs
                inv = 1.0 / (probs * rest)
                live = codes < 3
                codes_f = codes.astype(F32)
                a = jnp.where(live, codes_f, 0.0) * (rest * inv)
                bb = jnp.where(live, 2.0 - codes_f, 0.0) * (probs * inv)
                ah, al = split(a, 2)
                bh, bl = split(bb, 2)
                q2 = q2_ref[:, here]
                q22 = jnp.concatenate([q2, q2], axis=1)
                sum_a = sum_a + dot(q22, jnp.concatenate([ah, al], axis=0))
                sum_b = sum_b + dot(q22, jnp.concatenate([bh, bl], axis=0))
                sq_acc[b] = sq_acc[b] + lax.dot_general(
                    fgs_ref[...], jnp.concatenate([ah, al, bh, bl], axis=1), (((1,), (1,)), ((), ())),
                    preferred_element_type=F32)
            sum_a = (sum_a[0:PAD] + sum_a[PAD:2 * PAD])[0:pops]
            sum_b = (sum_b[0:PAD] + sum_b[PAD:2 * PAD])[0:pops]
            for i in range(per):
                cut = slice(i * wf, (i + 1) * wf)
                sf_send[it, c * per + i] = jnp.concatenate([sum_a[:, cut], sum_b[:, cut]], axis=1)
            for p in smp_peers[t]:
                start(smp_copy(sf_send.at[it, p], sf_recv, it, sf_ss, sf_rs, p, js))

        sum_q = jnp.concatenate([x[0:PAD] + x[PAD:2 * PAD] for x in sq_acc], axis=1)[0:pops]
        for v in range(nv):
            sq_send[it, v] = sum_q[:, v * ws:(v + 1) * ws]
        for p in var_peers:
            start(var_copy(sq_send.at[it, p], sq_recv, it, sq_ss, sq_rs, p, iv))

        total = sq_send[it, iv]
        for p in var_peers:
            var_copy(sq_send.at[it, p], sq_recv, it, sq_ss, sq_rs, p, p).wait_recv()
            total = total + sq_recv[it, p]
        numer = q_own * total
        q_own = (numer + 0.5) / (jnp.sum(numer, axis=0, keepdims=True) + 0.5 * pops)
        if last:
            shares_out[...] = q_own
        else:
            q_slots[it + 1, iv] = q_own
            for p in var_peers:
                start(var_copy(q_slots.at[it + 1, iv], q_slots, it + 1, q_ss, q_rs, p, iv))

        total = sf_send[it, js]
        for t in range(chunks):
            for p in smp_peers[t]:
                smp_copy(sf_send.at[it, p], sf_recv, it, sf_ss, sf_rs, p, p).wait_recv()
                total = total + sf_recv[it, p]
        alt_part = f_own * total[:, 0:wf]
        ref_part = (1.0 - f_own) * total[:, wf:2 * wf]
        f_own = (alt_part + 0.5) / (alt_part + ref_part + 1.0)
        if last:
            freqs_out[...] = f_own
        else:
            f_slots[it + 1, js] = f_own
            for p in all_smp:
                start(smp_copy(f_slots.at[it + 1, js], f_slots, it + 1, f_ss, f_rs, p, js))

    for copy in sent:
        copy.wait_send()


def hand_out(shares_ref, freqs_ref, shares_out, freqs_out):
    shares_out[...] = shares_ref[...]
    freqs_out[...] = freqs_ref[...]


def body(nv, ns, dosage, shares_init, freqs_init):
    pops, ws = shares_init.shape
    wf = freqs_init.shape[1]
    words, variants = dosage.shape
    samples = words * CODES
    chunk = variants // 2
    vmem = pl.BlockSpec(memory_space=pltpu.VMEM)
    hbm = pl.BlockSpec(memory_space=pl.ANY)
    dma = pltpu.SemaphoreType.DMA
    shapes = (jax.ShapeDtypeStruct((pops, ws), F32), jax.ShapeDtypeStruct((pops, wf), F32))
    shares, freqs = pl.pallas_call(
        functools.partial(em_kernel, nv, ns, chunk),
        out_shape=shapes,
        in_specs=[hbm, hbm, hbm],
        out_specs=(vmem, vmem),
        scratch_shapes=[
            pltpu.VMEM((words, variants), jnp.int32),
            pltpu.VMEM((pops, ws), F32),
            pltpu.VMEM((pops, wf), F32),
            pltpu.VMEM((ITERS, nv, pops, ws), F32),
            pltpu.VMEM((ITERS, ns, pops, wf), F32),
            pltpu.VMEM((ITERS, nv, pops, ws), F32),
            pltpu.VMEM((ITERS, nv, pops, ws), F32),
            pltpu.VMEM((ITERS, ns, pops, 2 * wf), F32),
            pltpu.VMEM((ITERS, ns, pops, 2 * wf), F32),
            pltpu.VMEM((PAD, samples), F32),
            pltpu.VMEM((PAD, chunk), F32),
            pltpu.VMEM((samples, 8 * PAD), BF16),
            pltpu.VMEM((2 * PAD, samples), BF16),
            pltpu.VMEM((8 * PAD, chunk), BF16),
            pltpu.VMEM((2 * PAD, 4 * chunk), BF16),
            dma((4,)),
            dma((ITERS, nv)), dma((ITERS, nv)),
            dma((ITERS, ns)), dma((ITERS, ns)),
            dma((ITERS, nv)), dma((ITERS, nv)),
            dma((ITERS, ns)), dma((ITERS, ns)),
        ],
        compiler_params=pltpu.CompilerParams(collective_id=0, has_side_effects=True),
        cost_estimate=pl.CostEstimate(flops=200000000, bytes_accessed=400000, transcendentals=1000000),
    )(dosage, shares_init, freqs_init)
    return pl.pallas_call(
        hand_out, out_shape=shapes, in_specs=[vmem, vmem], out_specs=(vmem, vmem),
    )(shares, freqs)


def solution(mesh):
    placed = (P("smp", "var"), P(None, ("smp", "var")), P(None, ("var", "smp")))
    return jax.shard_map(
        functools.partial(body, mesh.shape["var"], mesh.shape["smp"]),
        mesh=mesh,
        in_specs=placed,
        out_specs=(P(None, ("smp", "var")), P(None, ("var", "smp"))),
        check_vma=False,
    )
```
